32 devices in a mesh: dp: 8 (over z, x), tensor: 4 (over y, core).
Axes of the slice: x: 2, y: 2, z: 4, core: 2. Of those that a mesh axis runs over, the one named last changes fastest.
Arguments:
- out_first: bfloat16 [8, 197, 1024], P('dp', None, 'tensor'), may hold values from -6 to 6
- out_second: bfloat16 [8, 197, 1024], P('dp', None, 'tensor'), may hold values from -6 to 6
- grad_first: bfloat16 [8, 197, 1024], P('dp', None, 'tensor'), may hold values from -6 to 6
- grad_second: bfloat16 [8, 197, 1024], P('dp', None, 'tensor'), may hold values from -6 to 6
- gain_attn: float32 [1024], replicated, may hold values from 0.25 to 1.75
- gain_mlp: float32 [1024], replicated, may hold values from 0.25 to 1.75
- qkv_weight: bfloat16 [1024, 3, 1024], P(None, None, 'tensor'), may hold values from -1 to 1
- proj_weight: bfloat16 [1024, 1024], P(None, 'tensor'), may hold values from -0.1875 to 0.1875
- inner_weight: bfloat16 [1024, 4096], P(None, 'tensor'), may hold values from -0.1875 to 0.1875
- inner_bias: float32 [4096], P('tensor'), may hold values from -3 to 3
- outer_weight: bfloat16 [1024, 4096], P(None, 'tensor'), may hold values from -0.09375 to 0.09375
Outputs:
- input_first: bfloat16 [8, 197, 1024], P('dp', None, 'tensor')
- input_second: bfloat16 [8, 197, 1024], P('dp', None, 'tensor')
- back_first: bfloat16 [8, 197, 1024], P('dp', None, 'tensor')
- back_second: bfloat16 [8, 197, 1024], P('dp', None, 'tensor')
- grad_qkv: float32 [1024, 3, 1024], P('dp', None, 'tensor')
- grad_proj: float32 [1024, 1024], P('dp', 'tensor')
- grad_inner: float32 [1024, 4096], P('dp', 'tensor')
- grad_bias: float32 [4096], P('tensor')
- grad_outer: float32 [1024, 4096], P('dp', 'tensor')
- grad_gain_attn: float32 [1024], P('tensor')
- grad_gain_mlp: float32 [1024], P('tensor')
The draws below stay inside these ranges and needn't reach their ends.
All inputs are finite; a program needn't handle non-finite values.
Results may differ from the reference program's by a relative error of at most 0.016.
Values may be sent and summed in bfloat16 or wider, within the bound.
A program may use at most 64 MiB of HBM per device.

```python
import jax
import jax.numpy as jnp
from jax import lax

D = 1024
HEADS = 16
FF = 4096
SEQ = 197
IMAGES = 8


def draw_qkv_weight(key, part):
    base_key = jax.random.fold_in(key, 0)
    base_draw = jax.random.truncated_normal(base_key, -6.0, 6.0, (D, 3, D), jnp.float32) / D ** 0.5
    return jnp.clip(base_draw, -1.0, 1.0).astype(jnp.bfloat16)


def strengthened(array, own_key, source, target, blocks, factor):
    def block_of(axis_at):
        return (jnp.arange(array.shape[axis_at]) // (array.shape[axis_at] // blocks)).reshape((-1,) + (1,) * (array.ndim - 1 - axis_at))

    first = jax.random.permutation(own_key, blocks)[block_of(target)]
    other_side = (block_of(target) + blocks // 2) % blocks
    return jnp.where((block_of(source) == first) | (block_of(source) == other_side), factor * array, array)


def steps_of(key, shape, cuts, least, high):
    level = 1.0
    for axis_at, shards_of in cuts:
        heights = jax.random.uniform(jax.random.fold_in(jax.random.fold_in(key, 6), axis_at), (shards_of,), jnp.float32, least / len(cuts), high / len(cuts))
        level = level * jnp.repeat(jnp.exp(heights), shape[axis_at] // shards_of).reshape((-1,) + (1,) * (len(shape) - 1 - axis_at))
    return level


def noise(rng, shape, deviation, limit, cuts=(), dtype=jnp.bfloat16):
    values = jax.random.normal(rng, shape, jnp.float32) * deviation
    if len(cuts) > 0:
        values = steps_of(rng, shape, cuts, -0.22, 0.18) * values
    return jnp.clip(values, min=-limit, max=limit).astype(dtype)


def heavy_noise(own_key, shape, deviation, limit, pieces, heavy, kind=jnp.bfloat16):
    array = deviation * jax.random.normal(own_key, shape, jnp.float32)
    if pieces:
        array = array * steps_of(own_key, shape, pieces, -0.22, 0.18)
    return jnp.clip(strengthened(array, jax.random.fold_in(own_key, 3), *heavy), -limit, limit).astype(kind)


def setup_inputs(seed: int = 0) -> dict:
    keys = jax.random.split(jax.random.key(seed), 12)
    out_first = noise(keys[0], (IMAGES, SEQ, D), 1.0, 6.0, ((0, 8), (2, 4)))
    out_second = noise(keys[1], (IMAGES, SEQ, D), 1.0, 6.0, ((0, 8), (2, 4)))
    grad_first = noise(keys[2], (IMAGES, SEQ, D), 1.0, 6.0, ((0, 8), (2, 4)))
    grad_second = heavy_noise(keys[3], (IMAGES, SEQ, D), 1.0, 6.0, ((0, 8), (2, 4)), (0, 2, 8, 2.0))
    gain_attn = jnp.clip(1.0 + 0.15 * jax.random.normal(keys[4], (D,), jnp.float32), 0.25, 1.75)
    gain_mlp = jnp.clip(1.0 + 0.15 * jax.random.normal(keys[5], (D,), jnp.float32), 0.25, 1.75)
    qkv_weight = draw_qkv_weight(jax.random.fold_in(keys[11], 71), 0)
    proj_weight = noise(keys[7], (D, D), D ** -0.5, 0.1875, ((1, 4),))
    inner_weight = noise(keys[8], (D, FF), D ** -0.5, 0.1875, ((1, 4),))
    inner_bias = noise(keys[9], (FF,), 0.5, 3.0, ((0, 4),), jnp.float32)
    outer_weight = noise(keys[10], (D, FF), FF ** -0.5, 0.09375, ((1, 4),))
    return {"out_first": out_first, "out_second": out_second, "grad_first": grad_first, "grad_second": grad_second, "gain_attn": gain_attn, "gain_mlp": gain_mlp, "qkv_weight": qkv_weight, "proj_weight": proj_weight, "inner_weight": inner_weight, "inner_bias": inner_bias, "outer_weight": outer_weight}


epsilon = 1e-06

def normalize(values):
    centre = values - lax.optimization_barrier(jnp.mean(values, -1, keepdims=True))
    spread = lax.rsqrt(lax.optimization_barrier(jnp.mean(centre * centre, -1, keepdims=True)) + epsilon)
    return (centre * spread, spread)

def norm_back(grad_in, normed, spread, gain):
    scaled = grad_in * gain
    first_mean = lax.optimization_barrier(jnp.mean(scaled, -1, keepdims=True))
    second_mean = lax.optimization_barrier(jnp.mean(scaled * normed, -1, keepdims=True))
    return spread * (scaled - first_mean - normed * second_mean)

def image_attention(members):
    queries = members[0].astype(jnp.float32)
    key_rows = members[1].astype(jnp.float32)
    value_rows = members[2].astype(jnp.float32)
    grad_heads = members[3].astype(jnp.float32)
    factor = (D // HEADS) ** (-0.5)
    scores = jnp.einsum('qhe,khe->hqk', queries, key_rows) * factor
    attn_probs = jax.nn.softmax(scores, -1)
    probs_low = attn_probs.astype(jnp.bfloat16)
    probs_wide = probs_low.astype(jnp.float32)
    heads_out = jnp.einsum('hqk,khe->qhe', probs_wide, value_rows).astype(jnp.bfloat16)
    grad_probs = jnp.einsum('qhe,khe->hqk', grad_heads, value_rows)
    grad_value = jnp.einsum('hqk,qhe->khe', probs_wide, grad_heads).astype(jnp.bfloat16)
    row_dot = lax.optimization_barrier(jnp.sum(grad_probs * attn_probs, -1, keepdims=True))
    grad_scores = (attn_probs * (grad_probs - row_dot)).astype(jnp.bfloat16).astype(jnp.float32)
    grad_query = (jnp.einsum('hqk,khe->qhe', grad_scores, key_rows) * factor).astype(jnp.bfloat16)
    grad_key = (jnp.einsum('hqk,qhe->khe', grad_scores, queries) * factor).astype(jnp.bfloat16)
    return (heads_out, grad_query, grad_key, grad_value)

def reference(out_first, out_second, grad_first, grad_second, gain_attn, gain_mlp, qkv_weight, proj_weight, inner_weight, inner_bias, outer_weight):
    rows_all = IMAGES * SEQ
    head_dim = D // HEADS
    first_rows = out_first.reshape(rows_all, D).astype(jnp.float32)
    second_rows = out_second.reshape(rows_all, D).astype(jnp.float32)
    upper_grad = grad_first.reshape(rows_all, D).astype(jnp.float32)
    lower_grad = grad_second.reshape(rows_all, D)
    normed_mlp, spread_mlp = normalize(first_rows)
    input_mlp = (normed_mlp * gain_mlp).astype(jnp.bfloat16)
    hidden = jnp.dot(input_mlp, inner_weight, preferred_element_type=jnp.float32) + inner_bias
    active = jax.nn.gelu(hidden).astype(jnp.bfloat16)
    mlp_out = jnp.dot(active, outer_weight.T, preferred_element_type=jnp.float32)
    input_second = (second_rows - mlp_out).astype(jnp.bfloat16)
    grad_active = jnp.dot(lower_grad, outer_weight, preferred_element_type=jnp.float32)
    grad_hidden = jax.vjp(jax.nn.gelu, hidden)[1](grad_active)[0].astype(jnp.bfloat16)
    grad_outer = jnp.dot(lower_grad.T, active, preferred_element_type=jnp.float32)
    grad_inner = jnp.dot(input_mlp.T, grad_hidden, preferred_element_type=jnp.float32)
    grad_bias = lax.optimization_barrier(jnp.sum(grad_hidden.astype(jnp.float32), 0))
    grad_norm_mlp = jnp.dot(grad_hidden, inner_weight.T, preferred_element_type=jnp.float32)
    grad_gain_mlp = lax.optimization_barrier(jnp.sum(grad_norm_mlp * normed_mlp, 0))
    back_first = (upper_grad + norm_back(grad_norm_mlp, normed_mlp, spread_mlp, gain_mlp)).astype(jnp.bfloat16)
    normed_attn, spread_attn = normalize(input_second.astype(jnp.float32))
    input_attn = (normed_attn * gain_attn).astype(jnp.bfloat16)
    qkv_rows = jnp.einsum('td,dcj->tcj', input_attn.astype(jnp.float32), qkv_weight.astype(jnp.float32)).astype(jnp.bfloat16)
    grad_heads = jnp.dot(back_first, proj_weight, preferred_element_type=jnp.float32).astype(jnp.bfloat16)
    shaped = qkv_rows.reshape(IMAGES, SEQ, 3, HEADS, head_dim)
    heads_out, grad_query, grad_key, grad_value = lax.map(image_attention, (shaped[:, :, 0], shaped[:, :, 1], shaped[:, :, 2], grad_heads.reshape(IMAGES, SEQ, HEADS, head_dim)))
    attn_rows = heads_out.reshape(rows_all, D)
    grad_rows = jnp.stack([grad_query, grad_key, grad_value], 2).reshape(rows_all, 3, D)
    attn_out = jnp.dot(attn_rows, proj_weight.T, preferred_element_type=jnp.float32)
    input_first = (first_rows - attn_out).astype(jnp.bfloat16)
    grad_proj = jnp.dot(back_first.T, attn_rows, preferred_element_type=jnp.float32)
    grad_qkv = jnp.einsum('td,tcj->dcj', input_attn.astype(jnp.float32), grad_rows.astype(jnp.float32))
    grad_norm_attn = jnp.einsum('tcj,dcj->td', grad_rows.astype(jnp.float32), qkv_weight.astype(jnp.float32))
    grad_gain_attn = lax.optimization_barrier(jnp.sum(grad_norm_attn * normed_attn, 0))
    back_second = (lower_grad.astype(jnp.float32) + norm_back(grad_norm_attn, normed_attn, spread_attn, gain_attn)).astype(jnp.bfloat16)
    shape_out = (IMAGES, SEQ, D)
    return (input_first.reshape(shape_out), input_second.reshape(shape_out), back_first.reshape(shape_out), back_second.reshape(shape_out), grad_qkv, grad_proj, grad_inner, grad_bias, grad_outer, grad_gain_attn, grad_gain_mlp)
```

```python
import functools

import jax
import jax.numpy as jnp
from jax import lax
from jax.experimental import pallas as pl
from jax.experimental.pallas import tpu as pltpu
from jax.sharding import PartitionSpec as P

epsilon = 1e-06
HEAD = 64
BF = jnp.bfloat16
F32 = jnp.float32
MESH = pl.DeviceIdType.MESH
LIMIT = 61 * 2**20


def dot(a, b, dims=((1,), (0,))):
    return lax.dot_general(a, b, (dims, ((), ())), preferred_element_type=F32)


NT = ((1,), (1,))
TN = ((0,), (0,))


def kernel(
    sizes,
    of_ref, os_ref, gf_ref, gs_ref, gain_attn, gain_mlp, bias,
    qkv_hbm, proj_hbm, inner_hbm, outer_hbm,
    o_if, o_is, o_bf, o_bs, o_qkv, o_proj, o_inner, o_ga, o_gm, o_bias, o_outer,
    w_qkv, w_proj, w_inner, w_outer,
    g_in, g_is, g_back,
    a_mlp, a_more, a_attn, n_mlp, n_attn,
    dgelu, plain, qkv, gheads, probs, u_mlp, u_attn,
    at, lr, atm, at_tmp,
    r_act, r_gh, r_attn, r_rows,
    rs_s1, rs_r1, rs_k, rs_s2, rs_r2,
    st_s, st_r, sm_s, sm_r,
    *rest,
):
    groups, length, width, full, hid, tile, rows, near = sizes
    bits = groups.bit_length() - 1
    shard = full // groups
    m = groups // 2
    upper = groups // (2 * near)
    block = 2 * shard
    near_bits = near.bit_length() - 1
    pieces = rest[:-3]
    ssem, rsem, wsem = rest[-3:]
    d = lax.axis_index("dp")
    me = lax.axis_index("tensor")
    core, yy = me % 2, me // 2
    tc = yy * 2 + 1 - core
    ty = (1 - yy) * 2 + core
    td = (1 - yy) * 2 + 1 - core
    bit = [(d // 2**k) % 2 for k in range(bits)]
    step = [(1 - 2 * bit[k]) * 2**k for k in range(bits)]
    partner = [d + step[k] for k in range(bits)]
    place = (d // 2) % near

    def peer(r):
        return d + sum(step[1 + k] for k in range(near_bits) if r // 2**k % 2)

    counter = [0]
    pending = []

    def send(src, dst, dp_id, t_id):
        k = counter[0]
        counter[0] += 1
        c = pltpu.make_async_remote_copy(
            src_ref=src, dst_ref=dst, send_sem=ssem.at[k], recv_sem=rsem.at[k],
            device_id=(dp_id, t_id), device_id_type=MESH,
        )
        c.start()
        pending.append(c)
        return c

    def cols(i):
        return pl.ds(pl.multiple_of(i * width, width), width)

    weights = []
    for i, (src, dst) in enumerate(
        [(inner_hbm, w_inner), (outer_hbm, w_outer), (qkv_hbm, w_qkv), (proj_hbm, w_proj)]
    ):
        c = pltpu.make_async_copy(src, dst, wsem.at[i])
        c.start()
        weights.append(c)

    barrier = pltpu.get_barrier_semaphore()
    peers = [(d, tc), (d, ty), (d, td)] + [(p, me) for p in partner]
    peers += [(peer(r), me) for r in range(1, near) if r.bit_count() > 1]
    for to in peers:
        pl.semaphore_signal(barrier, inc=1, device_id=to, device_id_type=MESH)

    def stage(g, src):
        g[:, cols(me)] = jnp.zeros((rows, width), BF)
        g[0:length, cols(me)] = src[0]

    g_of, g_low = g_in.at[0, 0], g_in.at[0, 1]
    stage(g_of, of_ref)
    stage(g_low, gs_ref)
    pl.semaphore_wait(barrier, len(peers))

    def ag_start(g):
        own = g.at[:, cols(me)]
        c2 = send(own, own, d, ty)
        c1 = send(own, own, d, tc)
        return [c1, c2]

    def ag_mid(g, cs):
        cs[1].wait_recv()
        far = g.at[:, cols(ty)]
        cs.append(send(far, far, d, tc))

    def ag_end(cs):
        cs[0].wait_recv()
        cs[2].wait_recv()

    def rs_start(i, part):
        rs_s1[i, 1] = part(td).astype(BF)
        c1 = send(rs_s1.at[i, 1], rs_r1.at[i, 1], d, tc)
        rs_k[i, 1] = part(ty)
        rs_s1[i, 0] = part(tc).astype(BF)
        c0 = send(rs_s1.at[i, 0], rs_r1.at[i, 0], d, tc)
        rs_k[i, 0] = part(me)
        return [c0, c1]

    def rs_mid(i, cs):
        cs[1].wait_recv()
        rs_s2[i] = (rs_k[i, 1] + rs_r1[i, 1].astype(F32)).astype(BF)
        cs.append(send(rs_s2.at[i], rs_r2.at[i], d, ty))

    def rs_end(i, cs):
        cs[0].wait_recv()
        cs[2].wait_recv()
        return rs_k[i, 0] + rs_r1[i, 0].astype(F32) + rs_r2[i].astype(F32)

    lane = lax.broadcasted_iota(jnp.int32, (rows, 128), 1)

    def stats_start(i, first, other):
        both = jnp.where(lane == 0, first, jnp.where(lane == 1, other, 0.0))
        st_s[i] = both.T[0:8]
        return [
            send(st_s.at[i], st_r.at[i, j], d, to) for j, to in enumerate((ty, td, tc))
        ]

    def stats_end(i, cs):
        for c in cs:
            c.wait_recv()
        total = st_s[i] + st_r[i, 0] + st_r[i, 1] + st_r[i, 2]
        both = total.T / full
        return both[:, 0:1], both[:, 1:2]

    def normalize(values):
        centre = values - jnp.mean(values, -1, keepdims=True)
        spread = lax.rsqrt(jnp.mean(centre * centre, -1, keepdims=True) + epsilon)
        return centre * spread, spread

    def two_parts(gain):
        wide = jnp.broadcast_to(gain, (16, full))
        high = wide.astype(BF).astype(F32)
        row = lax.broadcasted_iota(jnp.int32, (16, full), 0)
        return jnp.where(row == 0, high, wide - high).astype(BF)

    def left(i, a):
        at[i] = a[...].T.reshape(m, 2, shard, rows)
        part = pl.ds(core * (m // 2), m // 2)
        return send(at.at[i, part, 1 - bit[0]], lr.at[i, part], partner[0], me)

    def left_mid(i, c):
        c.wait_recv()
        part = pl.ds(core * (m // 2), m // 2)
        return send(lr.at[i, part], lr.at[i, part], d, tc)

    def right(r):
        return send(r.at[0], r.at[1], partner[0], me)

    def piece(p, i, r, cr):
        cr.wait_recv()
        keep = pieces[p][0]
        mine = at[i, :, bit[0]].reshape(m * shard, rows)
        theirs = lr[i].reshape(m * shard, rows)
        acc = dot(mine, r[0]) + dot(theirs, r[1])
        keep[...] = acc.reshape(m // 2, 2, shard, width)
        return halve(p, 0)

    def keep_left(r, kind, a):
        if upper == 1 and block % 128 == 0:
            at_c = pl.ds(pl.multiple_of(place * block, block), block)
            atm[kind, r] = a[:, at_c].T
        else:
            at_tmp[...] = a[...].T.reshape(upper, near, block, rows)
            atm[kind, r] = at_tmp[:, place].reshape(upper * block, rows)

    def mlp_piece(p, kind, x):
        keep = pieces[p][0]
        for j in range(hid // tile):
            c = slice(j * tile, (j + 1) * tile)
            acc = dot(atm[kind, 0], x[0, :, c])
            for r in range(1, near):
                acc = acc + dot(atm[kind, r], x[r, :, c])
            keep[:, :, :, c] = acc.reshape(upper, 2, shard, tile)
        return halve(p, 0)

    far_bits = list(range(1 + near_bits, bits))
    order = [[0] + far_bits] * 2 + [list(range(1, bits))] * 4
    outs = [o_outer, o_inner, o_qkv.at[0], o_qkv.at[1], o_qkv.at[2], o_proj]

    def bufs(p, s):
        return pieces[p][3 * s : 3 * s + 3]

    def halve(p, s):
        keep, out, into = bufs(p, s)
        k = order[p][s]
        out[...] = keep[:, 1 - bit[k]].astype(BF)
        return send(out, into, partner[k], me)

    def merge(p, s, c):
        c.wait_recv()
        keep, out, into = bufs(p, s)
        total = keep[:, bit[order[p][s]]] + into[...].astype(F32)
        if s == len(order[p]) - 1:
            outs[p][...] = total[0]
            return None
        nxt = bufs(p, s + 1)[0]
        nxt[...] = total.reshape(nxt.shape)
        return halve(p, s + 1)

    def gelu_parts(h):
        k0, k1 = 0.7978845608028654, 0.044715
        sq = h * h
        t = jnp.tanh(k0 * h * (1.0 + k1 * sq))
        active = (0.5 * h * (1.0 + t)).astype(BF)
        return active, 0.5 * (1.0 + t) + 0.5 * h * (1.0 - t * t) * (k0 * (1.0 + 3.0 * k1 * sq))

    tiles = [slice(j * tile, (j + 1) * tile) for j in range(hid // tile)]

    def image(r):
        normed, _ = normalize(g_in[r, 0].astype(F32))
        a_more[...] = (normed * gain_mlp[...]).astype(BF)
        keep_left(r, 0, a_more)
        keep_left(r, 1, g_in.at[r, 1])
        for c in tiles:
            h = dot(a_more[...], w_inner[:, c]) + bias[:, c]
            r_act[r, :, c], slope = gelu_parts(h)
            r_gh[r, :, c] = (dot(g_in[r, 1], w_outer[:, c]) * slope).astype(BF)

    c_of = ag_start(g_of)
    c_low = ag_start(g_low)
    own = g_in.at[0, :, :, cols(me)]
    c_z = [None] + [send(own, g_in.at[r, :, :, cols(me)], peer(r), me) for r in range(1, near)]
    weights[0].wait()
    for c in tiles:
        both = dot(two_parts(gain_mlp[...]), w_inner[:, c])
        u_mlp[:, c] = both[0:1] + both[1:2]
    ag_mid(g_of, c_of)
    ag_end(c_of)
    normed, sp_mlp = normalize(g_of[...].astype(F32))
    n_mlp[...] = normed
    a_mlp[...] = (normed * gain_mlp[...]).astype(BF)
    ag_mid(g_low, c_low)
    for c in tiles:
        h = dot(a_mlp[...], w_inner[:, c])
        plain[:, c] = h
        r_act[0, :, c], dgelu[:, c] = gelu_parts(h + bias[:, c])
    weights[1].wait()
    c_mlp = rs_start(0, lambda i: dot(r_act[0], w_outer[cols(i), :], NT))
    ag_end(c_low)
    first = jnp.zeros((rows, 1), F32)
    other = jnp.zeros((rows, 1), F32)
    for c in tiles:
        gl = (dot(g_low[...], w_outer[:, c]) * dgelu[:, c]).astype(BF)
        r_gh[0, :, c] = gl
        gl = gl.astype(F32)
        first = first + jnp.sum(gl * u_mlp[:, c], -1, keepdims=True)
        other = other + jnp.sum(gl * plain[:, c], -1, keepdims=True)
        sm_s[0, :, 2 * width + c.start : 2 * width + c.stop] = jnp.sum(gl, 0, keepdims=True)
    rs_mid(0, c_mlp)
    c_st = stats_start(0, first, other)
    c_gn = rs_start(1, lambda i: dot(r_gh[0], w_inner[cols(i), :], NT))
    keep_left(0, 1, g_low)
    keep_left(0, 0, a_mlp)
    rs_mid(1, c_gn)
    total = rs_end(0, c_mlp)
    second = (os_ref[0].astype(F32) - total[0:length]).astype(BF)
    o_is[0] = second
    g_is[:, cols(me)] = jnp.zeros((rows, width), BF)
    g_is[0:length, cols(me)] = second
    c_is = ag_start(g_is)
    total = rs_end(1, c_gn)
    first, other = stats_end(0, c_st)
    back = sp_mlp * (total * gain_mlp[:, cols(me)] - first - n_mlp[:, cols(me)] * other)
    back = (gf_ref[0].astype(F32) + back[0:length]).astype(BF)
    o_bf[0] = back
    g_back[:, cols(me)] = jnp.zeros((rows, width), BF)
    g_back[0:length, cols(me)] = back
    c_back = ag_start(g_back)
    sm_s[0, :, width : 2 * width] = jnp.sum(total * n_mlp[:, cols(me)], 0, keepdims=True)
    weights[2].wait()
    for j in range(3):
        both = dot(two_parts(gain_attn[...]), w_qkv[j])
        u_attn[j] = both[0:1] + both[1:2]
    ag_mid(g_is, c_is)
    ag_end(c_is)
    normed, sp_attn = normalize(g_is[...].astype(F32))
    n_attn[...] = normed[:, :]
    a_attn[...] = (normed * gain_attn[...]).astype(BF)
    for j in range(3):
        qkv[:, j * width : (j + 1) * width] = dot(a_attn[...], w_qkv[j]).astype(BF)
    factor = HEAD**-0.5
    valid = lax.broadcasted_iota(jnp.int32, (rows, rows), 1) < length
    heads = [slice(h * HEAD, (h + 1) * HEAD) for h in range(width // HEAD)]

    def part_of(j, c):
        return qkv[:, j * width + c.start : j * width + c.stop]

    for h, c in enumerate(heads):
        s = jnp.where(valid, dot(part_of(0, c), part_of(1, c), NT) * factor, -1e30)
        e = jnp.exp(s - jnp.max(s, -1, keepdims=True))
        p = e / jnp.sum(e, -1, keepdims=True)
        probs[h] = p
        r_attn[0, :, c] = dot(p.astype(BF), part_of(2, c)).astype(BF)
    x_attn_rows = right(r_attn)
    x_attn = left(0, a_attn)
    ag_mid(g_back, c_back)
    ag_end(c_back)
    weights[3].wait()
    gheads[...] = dot(g_back[...], w_proj[...]).astype(BF)
    for h, c in enumerate(heads):
        r_rows[2, 0, :, c] = dot(probs[h].astype(BF), gheads[:, c], TN).astype(BF)
    x_v = right(r_rows.at[2])
    x_back = left(1, g_back)
    for h, c in enumerate(heads):
        p = probs[h]
        gp = dot(gheads[:, c], part_of(2, c), NT)
        gs = (p * (gp - jnp.sum(gp * p, -1, keepdims=True))).astype(BF)
        r_rows[0, 0, :, c] = (dot(gs, part_of(1, c)) * factor).astype(BF)
        r_rows[1, 0, :, c] = (dot(gs, part_of(0, c), TN) * factor).astype(BF)
    x_r = [right(r_rows.at[0]), right(r_rows.at[1]), x_v]
    first = jnp.zeros((rows, 1), F32)
    other = jnp.zeros((rows, 1), F32)
    for j in range(3):
        r = r_rows[j, 0].astype(F32)
        first = first + jnp.sum(r * u_attn[j], -1, keepdims=True)
        c = slice(j * width, (j + 1) * width)
        other = other + jnp.sum(r * qkv[:, c].astype(F32), -1, keepdims=True)
    c_gna = rs_start(
        3,
        lambda i: dot(r_rows[0, 0], w_qkv[0, cols(i), :], NT)
        + dot(r_rows[1, 0], w_qkv[1, cols(i), :], NT)
        + dot(r_rows[2, 0], w_qkv[2, cols(i), :], NT),
    )
    c_out = rs_start(2, lambda i: dot(r_attn[0], w_proj[cols(i), :], NT))
    rs_mid(3, c_gna)
    c_st = stats_start(1, first, other)
    rs_mid(2, c_out)
    c_in = [None] * near
    for r in range(1, near):
        c_z[r].wait_recv()
        c_in[r] = [ag_start(g_in.at[r, 0]), ag_start(g_in.at[r, 1])]
    x_attn = left_mid(0, x_attn)
    x_back = left_mid(1, x_back)
    x_back.wait_recv()
    zs = [None] * 6
    zs[5] = piece(5, 1, r_attn, x_attn_rows)
    x_attn.wait_recv()
    zs[4] = piece(4, 0, r_rows.at[2], x_r[2])

    def collect(r):
        for a in range(2):
            ag_mid(g_in.at[r, a], c_in[r][a])
        for a in range(2):
            ag_end(c_in[r][a])
        image(r)

    zs[2] = piece(2, 0, r_rows.at[0], x_r[0])
    zs[3] = piece(3, 0, r_rows.at[1], x_r[1])
    zs[5] = merge(5, 0, zs[5])
    total = rs_end(3, c_gna)
    sm_s[0, :, 0:width] = jnp.sum(total * n_attn[:, cols(me)], 0, keepdims=True)
    c_sm = send(sm_s.at[0], sm_r.at[0], partner[0], me)
    first, other = stats_end(1, c_st)
    back = sp_attn * (
        total * gain_attn[:, cols(me)] - first - n_attn[:, cols(me)] * other
    )
    o_bs[0] = (gs_ref[0].astype(F32) + back[0:length]).astype(BF)
    total = rs_end(2, c_out)
    o_if[0] = (of_ref[0].astype(F32) - total[0:length]).astype(BF)
    zs[4] = merge(4, 0, zs[4])
    for r in range(1, near):
        collect(r)
    zs[0] = mlp_piece(0, 1, r_act)
    zs[1] = mlp_piece(1, 0, r_gh)
    for p in (2, 3):
        zs[p] = merge(p, 0, zs[p])
    for k in range(1, bits):
        c_sm.wait_recv()
        sm_s[k] = sm_s[k - 1] + sm_r[k - 1]
        c_sm = send(sm_s.at[k], sm_r.at[k], partner[k], me)
    for s in range(1, bits - 1):
        for p in (5, 4, 2, 3):
            zs[p] = merge(p, s, zs[p])
    for s in range(len(order[0])):
        for p in (0, 1):
            zs[p] = merge(p, s, zs[p])
    c_sm.wait_recv()
    small = sm_s[bits - 1] + sm_r[bits - 1]
    o_ga[...] = small[:, 0:width]
    o_gm[...] = small[:, width : 2 * width]
    o_bias[...] = small[:, 2 * width :]
    for c in pending:
        c.wait_send()


def hand_out(*refs):
    count = (len(refs) - 2) // 3
    source, target, held = refs[:count], refs[count : 2 * count], refs[2 * count : 3 * count]
    first = [pltpu.make_async_copy(source[i], held[i], refs[-2].at[i]) for i in range(count)]
    second = [pltpu.make_async_copy(held[i], target[i], refs[-1].at[i]) for i in range(count)]
    for c in first:
        c.start()
    for c, e in zip(first, second):
        c.wait()
        e.start()
    for e in second:
        e.wait()


def on_device(
    out_first, out_second, grad_first, grad_second, gain_attn, gain_mlp,
    qkv_weight, proj_weight, inner_weight, inner_bias, outer_weight,
):
    images, length, width = out_first.shape
    parts = lax.axis_size("tensor")
    groups = lax.axis_size("dp")
    full = width * parts
    hid = inner_weight.shape[1]
    rows = (length + 15) // 16 * 16
    shard = full // groups
    bits = groups.bit_length() - 1
    near = min(groups // 2, 4)
    sizes = (groups, length, width, full, hid, 256, rows, near)
    vm = pltpu.VMEM
    half = groups // 2
    upper = groups // (2 * near)
    block = 2 * shard
    scratch = [
        vm((3, full, width), BF), vm((full, width), BF), vm((full, hid), BF), vm((full, hid), BF),
    ]
    scratch += [vm((near, 2, rows, full), BF)] + [vm((rows, full), BF)] * 2
    scratch += [vm((rows, full), BF)] * 3
    scratch += [vm((rows, full), F32)] * 2
    scratch += [vm((rows, hid), F32), vm((rows, hid), F32), vm((rows, 3 * width), BF), vm((rows, width), BF)]
    scratch += [vm((width // HEAD, rows, rows), F32), vm((1, hid), F32), vm((3, 1, width), F32)]
    scratch += [vm((2, half, 2, shard, rows), BF), vm((2, half, shard, rows), BF)]
    scratch += [vm((2, near, upper * block, rows), BF), vm((upper, near, block, rows), BF)]
    scratch += [vm((near, rows, hid), BF), vm((near, rows, hid), BF), vm((2, rows, width), BF), vm((3, 2, rows, width), BF)]
    scratch += [
        vm((4, 2, rows, width), BF), vm((4, 2, rows, width), BF), vm((4, 2, rows, width), F32),
        vm((4, rows, width), BF), vm((4, rows, width), BF),
    ]
    scratch += [vm((2, 8, rows), F32), vm((2, 3, 8, rows), F32)]
    small = 2 * width + hid
    scratch += [vm((bits, 1, small), F32), vm((bits, 1, small), F32)]
    for n, k in ((hid, upper), (hid, upper)) + ((width, half // 2),) * 4:
        bufs = []
        while k >= 1:
            bufs += [vm((k, 2, shard, n), F32), vm((k, shard, n), BF), vm((k, shard, n), BF)]
            k //= 2
        scratch.append(bufs)
    scratch += [pltpu.SemaphoreType.DMA((120,)), pltpu.SemaphoreType.DMA((120,)), pltpu.SemaphoreType.DMA((4,))]
    local = jax.ShapeDtypeStruct((images, length, width), BF)
    out_shape = [
        local, local, local, local,
        jax.ShapeDtypeStruct((3, shard, width), F32),
        jax.ShapeDtypeStruct((shard, width), F32),
        jax.ShapeDtypeStruct((shard, hid), F32),
        jax.ShapeDtypeStruct((1, width), F32),
        jax.ShapeDtypeStruct((1, width), F32),
        jax.ShapeDtypeStruct((1, hid), F32),
        jax.ShapeDtypeStruct((shard, hid), F32),
    ]
    v = pl.BlockSpec(memory_space=pltpu.VMEM)
    a = pl.BlockSpec(memory_space=pl.ANY)
    hbm = pl.BlockSpec(memory_space=pltpu.HBM)
    o = pl.pallas_call(
        functools.partial(kernel, sizes),
        out_shape=out_shape,
        in_specs=[v] * 7 + [hbm] * 4,
        out_specs=[v] * 11,
        scratch_shapes=scratch,
        compiler_params=pltpu.CompilerParams(
            collective_id=0, has_side_effects=True, vmem_limit_bytes=LIMIT
        ),
    )(
        out_first, out_second, grad_first, grad_second,
        gain_attn.reshape(1, full), gain_mlp.reshape(1, full), inner_bias.reshape(1, hid),
        jnp.transpose(qkv_weight, (1, 0, 2)), proj_weight, inner_weight, outer_weight,
    )
    o = pl.pallas_call(
        hand_out,
        out_shape=out_shape,
        in_specs=[a] * 11,
        out_specs=[a] * 11,
        scratch_shapes=[vm(x.shape, x.dtype) for x in out_shape]
        + [pltpu.SemaphoreType.DMA((11,)), pltpu.SemaphoreType.DMA((11,))],
        compiler_params=pltpu.CompilerParams(vmem_limit_bytes=LIMIT),
    )(*o)
    return (
        o[0], o[1], o[2], o[3], jnp.transpose(o[4], (1, 0, 2)), o[5], o[6],
        o[9].reshape(hid), o[10], o[7].reshape(width), o[8].reshape(width),
    )


def solution(mesh):
    act = P("dp", None, "tensor")
    in_specs = (
        act, act, act, act, P(), P(), P(None, None, "tensor"), P(None, "tensor"),
        P(None, "tensor"), P("tensor"), P(None, "tensor"),
    )
    out_specs = (
        act, act, act, act, P("dp", None, "tensor"), P("dp", "tensor"), P("dp", "tensor"),
        P("tensor"), P("dp", "tensor"), P("tensor"), P("tensor"),
    )
    return jax.shard_map(
        on_device, mesh=mesh, in_specs=in_specs, out_specs=out_specs, check_vma=False
    )
```

```python
import functools

import jax
import jax.numpy as jnp
from jax import lax
from jax.experimental import pallas as pl
from jax.experimental.pallas import tpu as pltpu
from jax.sharding import PartitionSpec as P

epsilon = 1e-06
HEAD = 64
BF = jnp.bfloat16
F32 = jnp.float32
MESH = pl.DeviceIdType.MESH
LIMIT = 61 * 2**20


def dot(a, b, dims=((1,), (0,))):
    return lax.dot_general(a, b, (dims, ((), ())), preferred_element_type=F32)


NT = ((1,), (1,))
TN = ((0,), (0,))


def kernel(
    sizes,
    of_ref, os_ref, gf_ref, gs_ref, gain_attn, gain_mlp, bias,
    qkv_hbm, proj_hbm, inner_hbm, outer_hbm,
    o_if, o_is, o_bf, o_bs, o_qkv, o_proj, o_inner, o_ga, o_gm, o_bias, o_outer,
    w_qkv, w_proj, w_inner, w_outer,
    g_in, g_is, g_back,
    a_mlp, a_more, a_attn, n_mlp, n_attn,
    dgelu, plain, qkv, gheads, probs, u_mlp, u_attn,
    own_t, their_t, ls, lr, pt_s, pt_r, spare, atm, at_tmp,
    r_act, r_gh, r_attn, r_rows,
    rs_s1, rs_r1, rs_k, rs_s2, rs_r2,
    st_s, st_r, sm_s, sm_r,
    *rest,
):
    groups, length, width, full, hid, tile, rows, near = sizes
    bits = groups.bit_length() - 1
    shard = full // groups
    m = groups // 2
    mine = m * width // full
    upper = groups // (2 * near)
    block = 2 * shard
    near_bits = near.bit_length() - 1
    pieces = rest[:-3]
    ssem, rsem, wsem = rest[-3:]
    d = lax.axis_index("dp")
    me = lax.axis_index("tensor")
    core, yy = me % 2, me // 2
    tc = yy * 2 + 1 - core
    ty = (1 - yy) * 2 + core
    td = (1 - yy) * 2 + 1 - core
    bit = [(d // 2**k) % 2 for k in range(bits)]
    step = [(1 - 2 * bit[k]) * 2**k for k in range(bits)]
    partner = [d + step[k] for k in range(bits)]
    place = (d // 2) % near

    def peer(r):
        return d + sum(step[1 + k] for k in range(near_bits) if r // 2**k % 2)

    counter = [0]
    pending = []

    def send(src, dst, dp_id, t_id):
        k = counter[0]
        counter[0] += 1
        c = pltpu.make_async_remote_copy(
            src_ref=src, dst_ref=dst, send_sem=ssem.at[k], recv_sem=rsem.at[k],
            device_id=(dp_id, t_id), device_id_type=MESH,
        )
        c.start()
        pending.append(c)
        return c

    def cols(i):
        return pl.ds(pl.multiple_of(i * width, width), width)

    weights = []
    for i, (src, dst) in enumerate(
        [(inner_hbm, w_inner), (outer_hbm, w_outer), (qkv_hbm, w_qkv), (proj_hbm, w_proj)]
    ):
        c = pltpu.make_async_copy(src, dst, wsem.at[i])
        c.start()
        weights.append(c)

    barrier = pltpu.get_barrier_semaphore()
    peers = [(d, tc), (d, ty), (d, td)] + [(p, me) for p in partner]
    peers += [(peer(r), me) for r in range(1, near) if r.bit_count() > 1]
    for to in peers:
        pl.semaphore_signal(barrier, inc=1, device_id=to, device_id_type=MESH)

    def stage(g, src):
        g[:, cols(me)] = jnp.zeros((rows, width), BF)
        g[0:length, cols(me)] = src[0]

    g_of, g_low = g_in.at[0, 0], g_in.at[0, 1]
    stage(g_of, of_ref)
    stage(g_low, gs_ref)
    pl.semaphore_wait(barrier, len(peers))

    def ag_start(view):
        own = view(me)
        c2 = send(own, own, d, ty)
        c1 = send(own, own, d, tc)
        return [c1, c2]

    def ag_mid(view, cs):
        cs[1].wait_recv()
        far = view(ty)
        cs.append(send(far, far, d, tc))

    def ag_end(cs):
        cs[0].wait_recv()
        cs[2].wait_recv()

    def rs_start(i, part):
        rs_s1[i, 1] = part(td).astype(BF)
        c1 = send(rs_s1.at[i, 1], rs_r1.at[i, 1], d, tc)
        rs_k[i, 1] = part(ty)
        rs_s1[i, 0] = part(tc).astype(BF)
        c0 = send(rs_s1.at[i, 0], rs_r1.at[i, 0], d, tc)
        rs_k[i, 0] = part(me)
        return [c0, c1]

    def rs_mid(i, cs):
        cs[1].wait_recv()
        rs_s2[i] = (rs_k[i, 1] + rs_r1[i, 1].astype(F32)).astype(BF)
        cs.append(send(rs_s2.at[i], rs_r2.at[i], d, ty))

    def rs_end(i, cs):
        cs[0].wait_recv()
        cs[2].wait_recv()
        return rs_k[i, 0] + rs_r1[i, 0].astype(F32) + rs_r2[i].astype(F32)

    lane = lax.broadcasted_iota(jnp.int32, (rows, 128), 1)

    def as_rows(first, other):
        both = jnp.where(lane == 0, first, jnp.where(lane == 1, other, 0.0))
        return both.T[0:8]

    def stats_start(i, first, other):
        st_s[i] = as_rows(first, other)
        return [
            send(st_s.at[i], st_r.at[i, j], d, to) for j, to in enumerate((ty, td, tc))
        ]

    def stats_end(i, cs):
        for c in cs:
            c.wait_recv()
        total = st_s[i] + st_r[i, 0] + st_r[i, 1] + st_r[i, 2]
        both = total.T / full
        return both[:, 0:1], both[:, 1:2]

    def normalize(values):
        mean = jnp.mean(values, -1, keepdims=True)
        centre = values - mean
        spread = lax.rsqrt(jnp.mean(centre * centre, -1, keepdims=True) + epsilon)
        return centre * spread, spread, mean

    def two_parts(gain):
        wide = jnp.broadcast_to(gain, (16, full))
        high = wide.astype(BF).astype(F32)
        row = lax.broadcasted_iota(jnp.int32, (16, full), 0)
        return jnp.where(row == 0, high, wide - high).astype(BF)

    def pick(values, parity):
        if mine == 1:
            return jnp.where(parity == 0, values[:, :shard], values[:, shard:])
        t = values.T.reshape(mine, 2, shard, values.shape[0])
        t = jnp.where(parity == 0, t[:, 0], t[:, 1])
        return t.reshape(mine * shard, values.shape[0]).T

    def share(i, a):
        ls[i] = pick(a[:, cols(me)], 1 - bit[0])
        return send(ls.at[i], lr.at[i, me], partner[0], me)

    def shared(i):
        return lambda t: lr.at[i, t]

    def keep_theirs(i, moments=None):
        n = mine * shard
        for t in range(full // width):
            a = lr[i, t]
            if moments is not None:
                mean, spread = moments
                gain = jnp.broadcast_to(gain_attn[:, t * width : (t + 1) * width], (16, width))
                gain = pick(gain, bit[0])[0:1]
                a = ((a.astype(F32) - mean) * spread * gain).astype(BF)
            their_t[i, t * n : (t + 1) * n] = a.T

    def keep_own(i, a):
        if shard % 128 == 0:
            for j in range(m):
                at_c = pl.ds(pl.multiple_of((2 * j + bit[0]) * shard, shard), shard)
                own_t[i, j] = a[:, at_c].T
        else:
            spare[...] = a[...].T.reshape(m, 2, shard, rows)
            own_t[i] = spare[:, bit[0]]

    def right(r):
        return send(r.at[0], r.at[1], partner[0], me)

    def piece(p, i, r, cr):
        cr.wait_recv()
        keep = pieces[p][0]
        ours = own_t[i].reshape(m * shard, rows)
        acc = dot(ours, r[0]) + dot(their_t[i], r[1])
        keep[...] = acc.reshape(m // 2, 2, shard, width)
        return halve(p, 0)

    def keep_left(r, kind, a):
        if upper == 1 and block % 128 == 0:
            at_c = pl.ds(pl.multiple_of(place * block, block), block)
            atm[kind, r] = a[:, at_c].T
        else:
            at_tmp[...] = a[...].T.reshape(upper, near, block, rows)
            atm[kind, r] = at_tmp[:, place].reshape(upper * block, rows)

    def mlp_piece(p, kind, x):
        keep = pieces[p][0]
        for j in range(hid // tile):
            c = slice(j * tile, (j + 1) * tile)
            acc = dot(atm[kind, 0], x[0, :, c])
            for r in range(1, near):
                acc = acc + dot(atm[kind, r], x[r, :, c])
            keep[:, :, :, c] = acc.reshape(upper, 2, shard, tile)
        return halve(p, 0)

    far_bits = list(range(1 + near_bits, bits))
    order = [[0] + far_bits] * 2 + [list(range(1, bits))] * 4
    outs = [o_outer, o_inner, o_qkv.at[0], o_qkv.at[1], o_qkv.at[2], o_proj]

    def bufs(p, s):
        return pieces[p][3 * s : 3 * s + 3]

    def halve(p, s):
        keep, out, into = bufs(p, s)
        k = order[p][s]
        out[...] = keep[:, 1 - bit[k]].astype(BF)
        return send(out, into, partner[k], me)

    def merge(p, s, c):
        c.wait_recv()
        keep, out, into = bufs(p, s)
        total = keep[:, bit[order[p][s]]] + into[...].astype(F32)
        if s == len(order[p]) - 1:
            outs[p][...] = total[0]
            return None
        nxt = bufs(p, s + 1)[0]
        nxt[...] = total.reshape(nxt.shape)
        return halve(p, s + 1)

    def gelu_parts(h):
        k0, k1 = 0.7978845608028654, 0.044715
        sq = h * h
        t = jnp.tanh(k0 * h * (1.0 + k1 * sq))
        active = (0.5 * h * (1.0 + t)).astype(BF)
        return active, 0.5 * (1.0 + t) + 0.5 * h * (1.0 - t * t) * (k0 * (1.0 + 3.0 * k1 * sq))

    tiles = [slice(j * tile, (j + 1) * tile) for j in range(hid // tile)]

    def image(r):
        normed, _, _ = normalize(g_in[r, 0].astype(F32))
        a_more[...] = (normed * gain_mlp[...]).astype(BF)
        keep_left(r, 0, a_more)
        keep_left(r, 1, g_in.at[r, 1])
        for c in tiles:
            h = dot(a_more[...], w_inner[:, c]) + bias[:, c]
            r_act[r, :, c], slope = gelu_parts(h)
            r_gh[r, :, c] = (dot(g_in[r, 1], w_outer[:, c]) * slope).astype(BF)

    def whole_rows(g):
        return lambda t: g.at[:, cols(t)]

    def one_of(r, a):
        return whole_rows(g_in.at[r, a])

    def both_of(r):
        return lambda t: g_in.at[r, :, :, cols(t)]

    by_tensor = [r for r in (3, 2) if r < near]
    by_near = [1] if near > 1 else []
    v_of, v_low, v_is, v_back = map(whole_rows, (g_of, g_low, g_is, g_back))
    c_of = ag_start(v_of)
    c_z = [None] * near
    for r in by_near + by_tensor[:1]:
        c_z[r] = send(both_of(0)(me), both_of(r)(me), peer(r), me)
    weights[0].wait()
    for c in tiles:
        both = dot(two_parts(gain_mlp[...]), w_inner[:, c])
        u_mlp[:, c] = both[0:1] + both[1:2]
    c_low = ag_start(v_low)
    ag_mid(v_of, c_of)
    ag_end(c_of)
    normed, sp_mlp, _ = normalize(g_of[...].astype(F32))
    n_mlp[...] = normed
    a_mlp[...] = (normed * gain_mlp[...]).astype(BF)
    ag_mid(v_low, c_low)
    c_far = {r: send(both_of(0)(ty), both_of(r)(ty), peer(r), me) for r in by_near}
    for r in by_tensor[1:]:
        c_z[r] = send(both_of(0)(me), both_of(r)(me), peer(r), me)
        c_far[r] = send(v_of(ty), one_of(r, 0)(ty), peer(r), me)
    for c in tiles:
        h = dot(a_mlp[...], w_inner[:, c])
        plain[:, c] = h
        r_act[0, :, c], dgelu[:, c] = gelu_parts(h + bias[:, c])
    weights[1].wait()
    c_mlp = rs_start(0, lambda i: dot(r_act[0], w_outer[cols(i), :], NT))
    rs_mid(0, c_mlp)
    ag_end(c_low)
    first = jnp.zeros((rows, 1), F32)
    other = jnp.zeros((rows, 1), F32)
    for c in tiles:
        gl = (dot(g_low[...], w_outer[:, c]) * dgelu[:, c]).astype(BF)
        r_gh[0, :, c] = gl
        gl = gl.astype(F32)
        first = first + jnp.sum(gl * u_mlp[:, c], -1, keepdims=True)
        other = other + jnp.sum(gl * plain[:, c], -1, keepdims=True)
        sm_s[0, :, 2 * width + c.start : 2 * width + c.stop] = jnp.sum(gl, 0, keepdims=True)
    c_gn = rs_start(1, lambda i: dot(r_gh[0], w_inner[cols(i), :], NT))
    c_st = stats_start(0, first, other)
    rs_mid(1, c_gn)
    keep_left(0, 1, g_low)
    keep_left(0, 0, a_mlp)
    total = rs_end(0, c_mlp)
    second = (os_ref[0].astype(F32) - total[0:length]).astype(BF)
    o_is[0] = second
    g_is[:, cols(me)] = jnp.zeros((rows, width), BF)
    g_is[0:length, cols(me)] = second
    c_is = ag_start(v_is)
    x_attn = share(0, g_is)
    weights[2].wait()
    for j in range(3):
        both = dot(two_parts(gain_attn[...]), w_qkv[j])
        u_attn[j] = both[0:1] + both[1:2]
    total = rs_end(1, c_gn)
    first, other = stats_end(0, c_st)
    back = sp_mlp * (total * gain_mlp[:, cols(me)] - first - n_mlp[:, cols(me)] * other)
    back = (gf_ref[0].astype(F32) + back[0:length]).astype(BF)
    o_bf[0] = back
    g_back[:, cols(me)] = jnp.zeros((rows, width), BF)
    g_back[0:length, cols(me)] = back
    c_back = ag_start(v_back)
    x_back = share(1, g_back)
    sm_s[0, :, width : 2 * width] = jnp.sum(total * n_mlp[:, cols(me)], 0, keepdims=True)
    ag_mid(v_is, c_is)
    ag_end(c_is)
    c_in = {}

    def forward(view, t, c):
        c.wait_recv()
        return send(view(t), view(t), d, tc)

    x_attn.wait_recv()
    x_attn = ag_start(shared(0))
    for r in by_near:
        c_in[r] = [forward(both_of(r), me, c_z[r])]
    normed, sp_attn, mean = normalize(g_is[...].astype(F32))
    n_attn[...] = normed
    a_attn[...] = (normed * gain_attn[...]).astype(BF)
    pt_s[...] = as_rows(mean, sp_attn)
    c_pt = send(pt_s, pt_r, partner[0], me)
    for j in range(3):
        qkv[:, j * width : (j + 1) * width] = dot(a_attn[...], w_qkv[j]).astype(BF)
    factor = HEAD**-0.5
    valid = lax.broadcasted_iota(jnp.int32, (rows, rows), 1) < length
    heads = [slice(h * HEAD, (h + 1) * HEAD) for h in range(width // HEAD)]

    def part_of(j, c):
        return qkv[:, j * width + c.start : j * width + c.stop]

    for h, c in enumerate(heads):
        s = jnp.where(valid, dot(part_of(0, c), part_of(1, c), NT) * factor, -1e30)
        e = jnp.exp(s - jnp.max(s, -1, keepdims=True))
        p = e / jnp.sum(e, -1, keepdims=True)
        probs[h] = p
        r_attn[0, :, c] = dot(p.astype(BF), part_of(2, c)).astype(BF)
    x_attn_rows = right(r_attn)
    x_back.wait_recv()
    x_back = ag_start(shared(1))
    for r in by_tensor[:1]:
        c_z[r].wait_recv()
        c_in[r] = ag_start(both_of(r))
    ag_mid(v_back, c_back)
    ag_end(c_back)
    for r in by_tensor[1:]:
        c_z[r].wait_recv()
        c_in[r] = ag_start(one_of(r, 1))
        c_in[r].append(send(one_of(r, 0)(me), one_of(r, 0)(me), d, tc))
    weights[3].wait()
    gheads[...] = dot(g_back[...], w_proj[...]).astype(BF)
    for h, c in enumerate(heads):
        r_rows[2, 0, :, c] = dot(probs[h].astype(BF), gheads[:, c], TN).astype(BF)
    x_v = right(r_rows.at[2])
    for h, c in enumerate(heads):
        p = probs[h]
        gp = dot(gheads[:, c], part_of(2, c), NT)
        gs = (p * (gp - jnp.sum(gp * p, -1, keepdims=True))).astype(BF)
        r_rows[0, 0, :, c] = (dot(gs, part_of(1, c)) * factor).astype(BF)
        r_rows[1, 0, :, c] = (dot(gs, part_of(0, c), TN) * factor).astype(BF)
    x_r = [right(r_rows.at[0]), right(r_rows.at[1]), x_v]
    for r in by_near:
        c_in[r].append(forward(both_of(r), ty, c_far[r]))
    c_gna = rs_start(
        3,
        lambda i: dot(r_rows[0, 0], w_qkv[0, cols(i), :], NT)
        + dot(r_rows[1, 0], w_qkv[1, cols(i), :], NT)
        + dot(r_rows[2, 0], w_qkv[2, cols(i), :], NT),
    )
    ag_mid(shared(0), x_attn)
    ag_mid(shared(1), x_back)
    for r in by_near:
        for c in c_in[r]:
            c.wait_recv()
        image(r)
    rs_mid(3, c_gna)
    zs = [None] * 6
    keep_own(1, g_back)
    ag_end(x_back)
    keep_theirs(1)
    zs[5] = piece(5, 1, r_attn, x_attn_rows)
    keep_own(0, a_attn)
    c_pt.wait_recv()
    moments = pt_r[...].T
    ag_end(x_attn)
    keep_theirs(0, (moments[:, 0:1], moments[:, 1:2]))
    for r in by_tensor[:1]:
        ag_mid(both_of(r), c_in[r])
    zs[4] = piece(4, 0, r_rows.at[2], x_r[2])
    for r in by_tensor[1:]:
        c_in[r].append(forward(one_of(r, 0), ty, c_far[r]))
    for r in by_tensor[:1]:
        ag_end(c_in[r])
        image(r)
    zs[2] = piece(2, 0, r_rows.at[0], x_r[0])
    for r in by_tensor[1:]:
        cs = c_in[r]
        ag_mid(one_of(r, 1), cs)
    zs[3] = piece(3, 0, r_rows.at[1], x_r[1])
    total = rs_end(3, c_gna)
    sm_s[0, :, 0:width] = jnp.sum(total * n_attn[:, cols(me)], 0, keepdims=True)
    c_sm = send(sm_s.at[0], sm_r.at[0], partner[0], me)
    for r in by_tensor[1:]:
        for i in (0, 2, 3, 4):
            c_in[r][i].wait_recv()
        image(r)
    zs[0] = mlp_piece(0, 1, r_act)
    zs[1] = mlp_piece(1, 0, r_gh)

    def small_step(k):
        c_sm.wait_recv()
        sm_s[k] = sm_s[k - 1] + sm_r[k - 1]
        return send(sm_s.at[k], sm_r.at[k], partner[k], me)

    c_sm = small_step(1)
    zs[5] = merge(5, 0, zs[5])
    zs[4] = merge(4, 0, zs[4])
    c_out = rs_start(2, lambda i: dot(r_attn[0], w_proj[cols(i), :], NT))
    first = jnp.zeros((rows, 1), F32)
    other = jnp.zeros((rows, 1), F32)
    for j in range(3):
        r = r_rows[j, 0].astype(F32)
        first = first + jnp.sum(r * u_attn[j], -1, keepdims=True)
        c = slice(j * width, (j + 1) * width)
        other = other + jnp.sum(r * qkv[:, c].astype(F32), -1, keepdims=True)
    c_st = stats_start(1, first, other)
    rs_mid(2, c_out)
    zs[2] = merge(2, 0, zs[2])
    zs[3] = merge(3, 0, zs[3])
    first, other = stats_end(1, c_st)
    back = sp_attn * (
        total * gain_attn[:, cols(me)] - first - n_attn[:, cols(me)] * other
    )
    o_bs[0] = (gs_ref[0].astype(F32) + back[0:length]).astype(BF)
    total = rs_end(2, c_out)
    o_if[0] = (of_ref[0].astype(F32) - total[0:length]).astype(BF)
    for k in range(2, bits):
        c_sm = small_step(k)
    for s in range(1, bits - 1):
        for p in (5, 4, 2, 3):
            zs[p] = merge(p, s, zs[p])
    for s in range(len(order[0])):
        for p in (0, 1):
            zs[p] = merge(p, s, zs[p])
    c_sm.wait_recv()
    small = sm_s[bits - 1] + sm_r[bits - 1]
    o_ga[...] = small[:, 0:width]
    o_gm[...] = small[:, width : 2 * width]
    o_bias[...] = small[:, 2 * width :]
    for c in pending:
        c.wait_send()


def hand_out(*refs):
    count = (len(refs) - 2) // 3
    source, target, held = refs[:count], refs[count : 2 * count], refs[2 * count : 3 * count]
    first = [pltpu.make_async_copy(source[i], held[i], refs[-2].at[i]) for i in range(count)]
    second = [pltpu.make_async_copy(held[i], target[i], refs[-1].at[i]) for i in range(count)]
    for c in first:
        c.start()
    for c, e in zip(first, second):
        c.wait()
        e.start()
    for e in second:
        e.wait()


def on_device(
    out_first, out_second, grad_first, grad_second, gain_attn, gain_mlp,
    qkv_weight, proj_weight, inner_weight, inner_bias, outer_weight,
):
    images, length, width = out_first.shape
    parts = lax.axis_size("tensor")
    groups = lax.axis_size("dp")
    full = width * parts
    hid = inner_weight.shape[1]
    rows = (length + 15) // 16 * 16
    shard = full // groups
    bits = groups.bit_length() - 1
    near = min(groups // 2, 4)
    sizes = (groups, length, width, full, hid, 256, rows, near)
    vm = pltpu.VMEM
    half = groups // 2
    upper = groups // (2 * near)
    block = 2 * shard
    scratch = [
        vm((3, full, width), BF), vm((full, width), BF), vm((full, hid), BF), vm((full, hid), BF),
    ]
    scratch += [vm((near, 2, rows, full), BF)] + [vm((rows, full), BF)] * 2
    scratch += [vm((rows, full), BF)] * 3
    scratch += [vm((rows, full), F32)] * 2
    scratch += [vm((rows, hid), F32), vm((rows, hid), F32), vm((rows, 3 * width), BF), vm((rows, width), BF)]
    scratch += [vm((width // HEAD, rows, rows), F32), vm((1, hid), F32), vm((3, 1, width), F32)]
    mine = half // parts
    scratch += [vm((2, half, shard, rows), BF), vm((2, half * shard, rows), BF)]
    scratch += [vm((2, rows, mine * shard), BF), vm((2, parts, rows, mine * shard), BF)]
    scratch += [vm((8, rows), F32), vm((8, rows), F32), vm((half, 2, shard, rows), BF)]
    scratch += [vm((2, near, upper * block, rows), BF), vm((upper, near, block, rows), BF)]
    scratch += [vm((near, rows, hid), BF), vm((near, rows, hid), BF), vm((2, rows, width), BF), vm((3, 2, rows, width), BF)]
    scratch += [
        vm((4, 2, rows, width), BF), vm((4, 2, rows, width), BF), vm((4, 2, rows, width), F32),
        vm((4, rows, width), BF), vm((4, rows, width), BF),
    ]
    scratch += [vm((2, 8, rows), F32), vm((2, 3, 8, rows), F32)]
    small = 2 * width + hid
    scratch += [vm((bits, 1, small), F32), vm((bits, 1, small), F32)]
    for n, k in ((hid, upper), (hid, upper)) + ((width, half // 2),) * 4:
        bufs = []
        while k >= 1:
            bufs += [vm((k, 2, shard, n), F32), vm((k, shard, n), BF), vm((k, shard, n), BF)]
            k //= 2
        scratch.append(bufs)
    scratch += [pltpu.SemaphoreType.DMA((120,)), pltpu.SemaphoreType.DMA((120,)), pltpu.SemaphoreType.DMA((4,))]
    local = jax.ShapeDtypeStruct((images, length, width), BF)
    out_shape = [
        local, local, local, local,
        jax.ShapeDtypeStruct((3, shard, width), F32),
        jax.ShapeDtypeStruct((shard, width), F32),
        jax.ShapeDtypeStruct((shard, hid), F32),
        jax.ShapeDtypeStruct((1, width), F32),
        jax.ShapeDtypeStruct((1, width), F32),
        jax.ShapeDtypeStruct((1, hid), F32),
        jax.ShapeDtypeStruct((shard, hid), F32),
    ]
    v = pl.BlockSpec(memory_space=pltpu.VMEM)
    a = pl.BlockSpec(memory_space=pl.ANY)
    hbm = pl.BlockSpec(memory_space=pltpu.HBM)
    o = pl.pallas_call(
        functools.partial(kernel, sizes),
        out_shape=out_shape,
        in_specs=[v] * 7 + [hbm] * 4,
        out_specs=[v] * 11,
        scratch_shapes=scratch,
        compiler_params=pltpu.CompilerParams(
            collective_id=0, has_side_effects=True, vmem_limit_bytes=LIMIT
        ),
    )(
        out_first, out_second, grad_first, grad_second,
        gain_attn.reshape(1, full), gain_mlp.reshape(1, full), inner_bias.reshape(1, hid),
        jnp.transpose(qkv_weight, (1, 0, 2)), proj_weight, inner_weight, outer_weight,
    )
    o = pl.pallas_call(
        hand_out,
        out_shape=out_shape,
        in_specs=[a] * 11,
        out_specs=[a] * 11,
        scratch_shapes=[vm(x.shape, x.dtype) for x in out_shape]
        + [pltpu.SemaphoreType.DMA((11,)), pltpu.SemaphoreType.DMA((11,))],
        compiler_params=pltpu.CompilerParams(vmem_limit_bytes=LIMIT),
    )(*o)
    return (
        o[0], o[1], o[2], o[3], jnp.transpose(o[4], (1, 0, 2)), o[5], o[6],
        o[9].reshape(hid), o[10], o[7].reshape(width), o[8].reshape(width),
    )


def solution(mesh):
    act = P("dp", None, "tensor")
    in_specs = (
        act, act, act, act, P(), P(), P(None, None, "tensor"), P(None, "tensor"),
        P(None, "tensor"), P("tensor"), P(None, "tensor"),
    )
    out_specs = (
        act, act, act, act, P("dp", None, "tensor"), P("dp", "tensor"), P("dp", "tensor"),
        P("tensor"), P("dp", "tensor"), P("tensor"), P("tensor"),
    )
    return jax.shard_map(
        on_device, mesh=mesh, in_specs=in_specs, out_specs=out_specs, check_vma=False
    )
```
